32 devices in a mesh: var: 4 (over z), lat: 4 (over x, core), lon: 2 (over y).
Axes of the slice: x: 2, y: 2, z: 4, core: 2. Of those that a mesh axis runs over, the one named last changes fastest.
Arguments:
- state: bfloat16 [1, 256, 384, 1024], P(None, 'var', 'lat', 'lon'), may hold values from -6 to 6
- weights_in: bfloat16 [2, 256, 256], replicated, may hold values from -0.25 to 0.25
- bias_in: float32 [2, 256], replicated, may hold values from -3 to 3
- weights_out: bfloat16 [2, 256, 256], replicated, may hold values from -2 to 2
Outputs:
- field: bfloat16 [1, 256, 384, 1024], P(None, 'var', 'lat', 'lon')
- zonal: float32 [1, 256, 384], P(None, 'var', 'lat')
- energy: float32 [256], P('var')
The draws below stay inside these ranges and needn't reach their ends.
All inputs are finite; a program needn't handle non-finite values.
Results may differ from the reference program's by a relative error of at most 0.012.
Values may be sent and summed in bfloat16 or wider, within the bound.
A program may use at most 64 MiB of HBM per device.

```python
import math
import jax
import jax.numpy as jnp
from jax import lax

BATCH = 1
C = 256
HID = 256
LAT = 384
LON = 1024
MLAT = 96
MLON = 96


def levels(own_key, shape, split, smallest, high):
    gain = 1.0
    for dim, blocks in split:
        steps = jax.random.uniform(jax.random.fold_in(jax.random.fold_in(own_key, 6), dim), (blocks,), jnp.float32, smallest / len(split), high / len(split))
        gain = gain * jnp.repeat(jnp.exp(steps), shape[dim] // blocks).reshape((-1,) + (1,) * (len(shape) - 1 - dim))
    return gain


def gaussian(own_key, extent, deviation, reach, split=(), held_as=jnp.bfloat16):
    entries = deviation * jax.random.normal(own_key, extent, jnp.float32)
    if split:
        entries = entries * levels(own_key, extent, split, -0.22, 0.18)
    return jnp.clip(entries, -reach, reach).astype(held_as)


def setup_inputs(seed: int = 0) -> dict:
    arg_keys = jax.random.split(jax.random.key(seed), 5)
    state = gaussian(arg_keys[0], (BATCH, C, LAT, LON), 1.0, 6.0, ((1, 4), (2, 4), (3, 2)))
    weights_in = gaussian(arg_keys[1], (2, HID, C), (2 * C) ** -0.5, 0.25)
    bias_in = gaussian(arg_keys[2], (2, HID), 0.5, 3.0, (), jnp.float32)
    weights_out = gaussian(arg_keys[3], (2, C, HID), (HID // 32) ** -0.5, 2.0)
    return dict(state=state, weights_in=weights_in, bias_in=bias_in, weights_out=weights_out)


def lon_forward(first, count):
    index = first + jnp.arange(count, dtype=jnp.int32)
    modes = jnp.arange(MLON, dtype=jnp.int32)
    phase = index[:, None] * modes[None, :] % LON
    angle = phase.astype(jnp.float32) * (2.0 * math.pi / LON)
    scale = 1.0 / math.sqrt(LAT * LON)
    return (jnp.stack([jnp.cos(angle), -jnp.sin(angle)], 1) * scale).astype(jnp.bfloat16)

def lat_forward(first, count):
    freqs = jnp.arange(MLAT, dtype=jnp.int32) - MLAT // 2
    index = first + jnp.arange(count, dtype=jnp.int32)
    phase = jnp.mod(freqs[:, None] * index[None, :], LAT)
    angle = phase.astype(jnp.float32) * (2.0 * math.pi / LAT)
    cosine, sine = (jnp.cos(angle), jnp.sin(angle))
    return jnp.stack([jnp.stack([cosine, sine]), jnp.stack([-sine, cosine])])

def lat_inverse(first, count):
    freqs = jnp.arange(MLAT, dtype=jnp.int32) - MLAT // 2
    index = first + jnp.arange(count, dtype=jnp.int32)
    phase = jnp.mod(index[:, None] * freqs[None, :], LAT)
    angle = phase.astype(jnp.float32) * (2.0 * math.pi / LAT)
    cosine, sine = (jnp.cos(angle), jnp.sin(angle))
    return jnp.stack([jnp.stack([cosine, -sine]), jnp.stack([sine, cosine])]).astype(jnp.bfloat16)

def lon_inverse(first, count):
    modes = jnp.arange(MLON, dtype=jnp.int32)
    index = first + jnp.arange(count, dtype=jnp.int32)
    phase = modes[:, None] * index[None, :] % LON
    angle = phase.astype(jnp.float32) * (2.0 * math.pi / LON)
    factor = jnp.where(modes == 0, 1.0, 2.0).astype(jnp.float32)[:, None] / math.sqrt(LAT * LON)
    return jnp.stack([factor * jnp.cos(angle), -factor * jnp.sin(angle)]).astype(jnp.bfloat16)

def area_weights(first, count):
    index = first + jnp.arange(count, dtype=jnp.int32)
    return jnp.cos(math.pi * ((index.astype(jnp.float32) + 0.5) / LAT - 0.5))

def complex_block(pair):
    real_part, imag_part = (pair[0], pair[1])
    return jnp.stack([jnp.stack([real_part, -imag_part], 1), jnp.stack([imag_part, real_part], 1)], 0)

def reference(state, weights_in, bias_in, weights_out):
    ltab = lon_forward(0, LON).astype(jnp.float32)
    qtab = lat_forward(0, LAT)
    rtab = lat_inverse(0, LAT).astype(jnp.float32)
    htab = lon_inverse(0, LON).astype(jnp.float32)
    block_in = complex_block(weights_in).astype(jnp.float32)
    block_out = complex_block(weights_out).astype(jnp.float32)
    weights = area_weights(0, LAT)

    def single(sample):
        lonspec = jnp.einsum('cnl,lpk->pcnk', sample.astype(jnp.float32), ltab)
        spectrum = jnp.einsum('qpjn,pcnk->qcjk', qtab, lonspec, precision=lax.Precision.HIGHEST).astype(jnp.bfloat16)
        hidden = jnp.einsum('qhpc,pcjk->qhjk', block_in, spectrum.astype(jnp.float32)) + bias_in[:, :, None, None]
        hidden = jnp.maximum(hidden, 0.0).astype(jnp.bfloat16)
        mixed = jnp.einsum('qoph,phjk->qojk', block_out, hidden.astype(jnp.float32)).astype(jnp.bfloat16)
        latback = jnp.einsum('qpnj,pojk->qonk', rtab, mixed.astype(jnp.float32)).astype(jnp.bfloat16)
        result = jnp.einsum('ponk,pkl->onl', latback.astype(jnp.float32), htab)
        active = jax.nn.gelu(result, approximate=False)
        squares = lax.optimization_barrier(jnp.sum(lax.optimization_barrier(jnp.sum(active * active, -1)) * weights[None, :], -1))
        return (active.astype(jnp.bfloat16), lax.optimization_barrier(jnp.mean(active, -1)), squares)
    field, zonal, parts = lax.map(single, state)
    energy = lax.optimization_barrier(jnp.sum(parts, 0)) / (BATCH * LON * jnp.sum(weights))
    return (field, zonal, energy)
```

```python
import functools
import math

import jax
import jax.numpy as jnp
from jax import lax
from jax.experimental import pallas as pl
from jax.experimental.pallas import tpu as pltpu
from jax.sharding import PartitionSpec as P

LAT = 384
LON = 1024
MLAT = 96
MLON = 96


def lon_forward(first, count):
    index = first + jnp.arange(count, dtype=jnp.int32)
    modes = jnp.arange(MLON, dtype=jnp.int32)
    phase = index[:, None] * modes[None, :] % LON
    angle = phase.astype(jnp.float32) * (2.0 * math.pi / LON)
    scale = 1.0 / math.sqrt(LAT * LON)
    return (jnp.stack([jnp.cos(angle), -jnp.sin(angle)], 1) * scale).astype(jnp.bfloat16)


def lat_forward(first, count):
    freqs = jnp.arange(MLAT, dtype=jnp.int32) - MLAT // 2
    index = first + jnp.arange(count, dtype=jnp.int32)
    phase = jnp.mod(freqs[:, None] * index[None, :], LAT)
    angle = phase.astype(jnp.float32) * (2.0 * math.pi / LAT)
    cosine, sine = (jnp.cos(angle), jnp.sin(angle))
    return jnp.stack([jnp.stack([cosine, sine]), jnp.stack([-sine, cosine])])


def lat_inverse(first, count):
    freqs = jnp.arange(MLAT, dtype=jnp.int32) - MLAT // 2
    index = first + jnp.arange(count, dtype=jnp.int32)
    phase = jnp.mod(index[:, None] * freqs[None, :], LAT)
    angle = phase.astype(jnp.float32) * (2.0 * math.pi / LAT)
    cosine, sine = (jnp.cos(angle), jnp.sin(angle))
    return jnp.stack([jnp.stack([cosine, -sine]), jnp.stack([sine, cosine])]).astype(jnp.bfloat16)


def lon_inverse(first, count):
    modes = jnp.arange(MLON, dtype=jnp.int32)
    index = first + jnp.arange(count, dtype=jnp.int32)
    phase = modes[:, None] * index[None, :] % LON
    angle = phase.astype(jnp.float32) * (2.0 * math.pi / LON)
    factor = jnp.where(modes == 0, 1.0, 2.0).astype(jnp.float32)[:, None] / math.sqrt(LAT * LON)
    return jnp.stack([factor * jnp.cos(angle), -factor * jnp.sin(angle)]).astype(jnp.bfloat16)


def area_weights(first, count):
    index = first + jnp.arange(count, dtype=jnp.int32)
    return jnp.cos(math.pi * ((index.astype(jnp.float32) + 0.5) / LAT - 0.5))


def complex_block(pair):
    real_part, imag_part = (pair[0], pair[1])
    return jnp.stack(
        [jnp.stack([real_part, -imag_part], 1), jnp.stack([imag_part, real_part], 1)], 0
    )


def plain_body(state, weights_in, bias_in, weights_out):
    batch, cdev, latdev, londev = state.shape
    nlat = lax.axis_size("lat")
    nlon = lax.axis_size("lon")
    lat_first = lax.axis_index("lat") * latdev
    lon_first = lax.axis_index("lon") * londev
    modes_lat = MLAT // nlat
    modes_lon = MLON // nlon
    qtab = lat_forward(lat_first, latdev)
    qsplit = qtab.reshape(2, 2, nlat, modes_lat, latdev)
    lonpart = jnp.einsum(
        "bcnl,lpk->pbcnk", state, lon_forward(lon_first, londev), preferred_element_type=jnp.float32
    )
    lonsplit = lonpart.reshape(2, batch, cdev, latdev, nlon, modes_lon)
    partial_value = jnp.einsum(
        "qpIJn,pbcnKk->qbcIKJk", qsplit, lonsplit, precision=lax.Precision.HIGHEST
    )
    spectrum = lax.psum_scatter(
        partial_value.reshape(2, batch, cdev, -1), ("lat", "lon"), scatter_dimension=3, tiled=True
    )
    spectrum = spectrum.astype(jnp.bfloat16)
    block_in = complex_block(weights_in)
    block_out = complex_block(weights_out)
    whole = lax.all_gather(spectrum, "var", axis=2, tiled=True)
    owned = lax.dynamic_slice_in_dim(block_out, lax.axis_index("var") * cdev, cdev, 1)
    hidden = jnp.einsum("qhpc,pbcj->qbhj", block_in, whole, preferred_element_type=jnp.float32)
    hidden = jnp.maximum(hidden + bias_in[:, None, :, None], 0.0).astype(jnp.bfloat16)
    mixed = jnp.einsum("qoph,pbhj->qboj", owned, hidden, preferred_element_type=jnp.float32).astype(
        jnp.bfloat16
    )
    mixed = mixed.reshape(2, batch, cdev, modes_lat, modes_lon)
    rtab = lat_inverse(lat_first, latdev)
    table = rtab
    latback = jnp.einsum(
        "qpnj,pbcjk->qbcnk",
        table,
        lax.all_gather(mixed, "lat", axis=3, tiled=True),
        preferred_element_type=jnp.float32,
    ).astype(jnp.bfloat16)
    htab = lon_inverse(lon_first, londev)
    table = htab
    result = jnp.einsum(
        "pbcnk,pkl->bcnl",
        lax.all_gather(latback, "lon", axis=4, tiled=True),
        table,
        preferred_element_type=jnp.float32,
    )
    active = jax.nn.gelu(result, approximate=False)
    field = active.astype(jnp.bfloat16)
    weights = area_weights(lat_first, latdev)
    denominator = batch * LON * jnp.sum(area_weights(0, LAT))
    row_total = jnp.sum(active, -1)
    row_square = jnp.sum(active * active, -1)
    summed, squared = lax.psum((row_total, row_square), "lon")
    zonal = summed / LON
    local = jnp.sum(squared * weights[None, None, :], axis=(0, 2))
    energy = lax.psum(local, "lat") / denominator
    return (field, zonal, energy)

LANES = 128
MESH = pl.DeviceIdType.MESH


def pad_lanes(table):
    return jnp.pad(table, [(0, 0)] * (table.ndim - 1) + [(0, LANES - table.shape[-1])])


def forward_kernel(x_ref, e_ref, q_ref, out_ref):
    channels, rows, count = x_ref.shape
    lon = jnp.dot(
        x_ref[...].reshape(channels * rows, count), e_ref[...], preferred_element_type=jnp.float32
    ).astype(jnp.bfloat16)
    lon = lon.reshape(channels, rows, 2 * LANES)
    parts = []
    for c in range(channels):
        both = jnp.concatenate([lon[c, :, :LANES], lon[c, :, LANES:]], 0)
        parts.append(jnp.dot(q_ref[...], both, preferred_element_type=jnp.float32))
    out_ref[...] = jnp.swapaxes(jnp.stack(parts), 0, 1).astype(jnp.bfloat16)


def inverse_kernel(g_ref, r_ref, h_ref, field_ref, zonal_ref, square_ref):
    channels = g_ref.shape[1]
    rows = field_ref.shape[1]
    modes = jnp.swapaxes(g_ref[...].astype(jnp.float32), 0, 1).astype(jnp.bfloat16)
    for c in range(channels):
        lat = jnp.dot(r_ref[...], modes[c], preferred_element_type=jnp.float32).astype(jnp.bfloat16)
        both = jnp.concatenate([lat[:rows], lat[rows:]], 1)
        result = jnp.dot(both, h_ref[...], preferred_element_type=jnp.float32)
        active = (0.5 * result) * (1.0 + lax.erf(result * math.sqrt(0.5)))
        field_ref[c] = active.astype(jnp.bfloat16)
        zonal_ref[c, :] = jnp.sum(active, -1)
        square_ref[c, :] = jnp.sum(active * active, -1)


def exchange_kernel(
    sizes, p_ref, win_ref, bias_ref, wout_ref, out_ref,
    pair, sums, slots, spec, gathered, back,
    s_pair, r_pair, s_red, r_red, s_z, r_z, s_b, r_b, s_all, r_all, s_fwd, r_fwd,
):
    nvar, nlat, nlon = sizes
    v, lat, lon = lax.axis_index("var"), lax.axis_index("lat"), lax.axis_index("lon")
    upper, core = lat // 2, lax.rem(lat, 2)
    nupper = nlat // 2
    block = p_ref.shape[0] // (nlat * nlon)
    part = block // nvar
    offsets = [(a, b) for a in range(nupper) for b in range(nlon)]
    count = len(offsets)

    def chip(t, sign=1):
        a, b = offsets[t]
        return (
            lax.rem(upper + sign * a + nupper, nupper),
            lax.rem(lon + sign * b + nlon, nlon),
        )

    def rows(where, parity):
        a, b = where
        return pl.ds(((a * 2 + parity) * nlon + b) * block, block)

    def send(src, dst, ssem, rsem, target):
        return pltpu.make_async_remote_copy(
            src_ref=src, dst_ref=dst, send_sem=ssem, recv_sem=rsem,
            device_id=target, device_id_type=MESH,
        )

    sibling = {"lat": upper * 2 + 1 - core}

    def peer(t):
        a, b = chip(t)
        return {"lat": a * 2 + core, "lon": b}

    def other(d):
        return {"var": lax.rem(v + d, nvar)}

    barrier = pltpu.get_barrier_semaphore()
    targets = [sibling] + [peer(t) for t in range(1, count)] + [other(d) for d in range(1, nvar)]
    for target in targets:
        pl.semaphore_signal(barrier, inc=1, device_id=target, device_id_type=MESH)
    pl.semaphore_wait(barrier, len(targets))

    order = list(range(1, count))[::-1] + [0]
    pairs = {}
    for t in order:
        pairs[t] = send(
            p_ref.at[rows(chip(t), 1 - core)], pair.at[t], s_pair.at[t], r_pair.at[t], sibling
        )
        pairs[t].start()
    reds = {}
    for t in order:
        pairs[t].wait_recv()
        mine = p_ref[rows(chip(t), core)].astype(jnp.float32) + pair[t].astype(jnp.float32)
        sums[t] = mine.astype(jnp.bfloat16)
        if t:
            reds[t] = send(sums.at[t], slots.at[t - 1], s_red.at[t - 1], r_red.at[t - 1], peer(t))
            reds[t].start()
    for t in order[:-1]:
        reds[t].wait_recv()
    total = sums[0].astype(jnp.float32)
    for t in range(1, count):
        total = total + slots[t - 1].astype(jnp.float32)
    spec[...] = total.astype(jnp.bfloat16)
    zs = []
    for d in range(1, nvar):
        copy = send(
            spec.at[pl.ds(lax.rem(v + d, nvar) * part, part)], gathered.at[v],
            s_z.at[d - 1], r_z.at[d - 1], other(d),
        )
        copy.start()
        zs.append(copy)
    gathered[v] = spec[pl.ds(v * part, part)]
    for d in range(1, nvar):
        src = gathered.at[lax.rem(v - d + nvar, nvar)]
        send(src, src, s_z.at[d - 1], r_z.at[d - 1], other(d)).wait_recv()
    held = gathered[...]
    cdev = held.shape[2]
    cols = []
    for j in range(part // 2):
        cols.append(held[:, 2 * j : 2 * j + 2].reshape(nvar * 2 * cdev, LANES))
    spectrum = jnp.concatenate(cols, 1)
    hidden = jnp.dot(win_ref[...], spectrum, preferred_element_type=jnp.float32)
    hidden = jnp.maximum(hidden + bias_ref[...], 0.0).astype(jnp.bfloat16)
    mixed = jnp.dot(wout_ref[...], hidden, preferred_element_type=jnp.float32).astype(jnp.bfloat16)
    for j in range(part // 2):
        back[:, 2 * j : 2 * j + 2] = mixed[:, j * LANES : (j + 1) * LANES].reshape(nvar, 2, cdev, LANES)
    base = (lat * nlon + lon) * block
    bs = []
    for d in range(1, nvar):
        copy = send(
            back.at[lax.rem(v + d, nvar)], out_ref.at[pl.ds(base + v * part, part)],
            s_b.at[d - 1], r_b.at[d - 1], other(d),
        )
        copy.start()
        bs.append(copy)
    out_ref[pl.ds(base + v * part, part)] = back[v]
    for d in range(1, nvar):
        src = out_ref.at[pl.ds(base + lax.rem(v - d + nvar, nvar) * part, part)]
        send(src, src, s_b.at[d - 1], r_b.at[d - 1], other(d)).wait_recv()
    own = out_ref.at[pl.ds(base, block)]
    alls = []
    for t in order[:-1]:
        copy = send(own, own, s_all.at[t - 1], r_all.at[t - 1], peer(t))
        copy.start()
        alls.append(copy)
    fwd = [send(own, own, s_fwd.at[0], r_fwd.at[0], sibling)]
    fwd[0].start()
    for t in range(1, count):
        got = out_ref.at[rows(chip(t, -1), core)]
        send(got, got, s_all.at[t - 1], r_all.at[t - 1], peer(t)).wait_recv()
        copy = send(got, got, s_fwd.at[t], r_fwd.at[t], sibling)
        copy.start()
        fwd.append(copy)
    for t in range(count):
        got = out_ref.at[rows(chip(t, -1), 1 - core)]
        send(got, got, s_fwd.at[t], r_fwd.at[t], sibling).wait_recv()
    for copy in list(pairs.values()) + list(reds.values()) + zs + bs + alls + fwd:
        copy.wait_send()


def statistics_kernel(sizes, x_ref, zonal_ref, energy_ref, slots, s_sem, r_sem):
    nvar, nlat, nlon = sizes
    lat, lon = lax.axis_index("lat"), lax.axis_index("lon")
    offsets = [(a, b) for a in range(nlat) for b in range(nlon)][1:]

    def target(t):
        a, b = offsets[t]
        return {"lat": lax.rem(lat + a, nlat), "lon": lax.rem(lon + b, nlon)}

    barrier = pltpu.get_barrier_semaphore()
    for t in range(len(offsets)):
        pl.semaphore_signal(barrier, inc=1, device_id=target(t), device_id_type=MESH)
    pl.semaphore_wait(barrier, len(offsets))
    copies = []
    for t in range(len(offsets)):
        copy = pltpu.make_async_remote_copy(
            src_ref=x_ref, dst_ref=slots.at[t], send_sem=s_sem.at[t], recv_sem=r_sem.at[t],
            device_id=target(t), device_id_type=MESH,
        )
        copy.start()
        copies.append(copy)
    zonal = x_ref[...]
    energy = x_ref[...]
    for t, (a, _) in enumerate(offsets):
        copies[t].wait_recv()
        energy = energy + slots[t]
        if a == 0:
            zonal = zonal + slots[t]
    zonal_ref[...] = zonal
    energy_ref[...] = energy
    for copy in copies:
        copy.wait_send()


def kernel_body(sizes, state, weights_in, bias_in, weights_out):
    nvar, nlat, nlon = sizes
    batch, cdev, latdev, londev = state.shape
    lat_first = lax.axis_index("lat") * latdev
    lon_first = lax.axis_index("lon") * londev
    vmem = pl.BlockSpec(memory_space=pltpu.VMEM)
    step = 16
    bf16 = jnp.bfloat16
    etab = pad_lanes(lon_forward(lon_first, londev)).reshape(londev, 2 * LANES)
    qtab = lat_forward(lat_first, latdev).astype(bf16)
    qtab = qtab.transpose(2, 0, 1, 3).reshape(2 * MLAT, 2 * latdev)
    partial_value = pl.pallas_call(
        forward_kernel,
        grid=(cdev // step,),
        in_specs=[
            pl.BlockSpec((step, latdev, londev), lambda i: (i, 0, 0)),
            pl.BlockSpec(etab.shape, lambda i: (0, 0)),
            pl.BlockSpec(qtab.shape, lambda i: (0, 0)),
        ],
        out_specs=pl.BlockSpec((2 * MLAT, step, LANES), lambda i: (0, i, 0)),
        out_shape=jax.ShapeDtypeStruct((2 * MLAT, cdev, LANES), bf16),
        compiler_params=pltpu.CompilerParams(vmem_limit_bytes=40 * 2**20),
        name="forward",
    )(state[0], etab, qtab)

    hid = weights_in.shape[1]
    win = complex_block(weights_in).reshape(2, hid, 2, nvar, cdev)
    win = win.transpose(0, 1, 3, 2, 4).reshape(2 * hid, 2 * nvar * cdev)
    wout = complex_block(weights_out).reshape(2, nvar, cdev, 2 * hid)
    wout = wout.transpose(1, 0, 2, 3).reshape(2 * nvar * cdev, 2 * hid)
    chips = nlat * nlon // 2
    block = 2 * MLAT // (nlat * nlon)
    part = block // nvar
    dma = pltpu.SemaphoreType.DMA
    whole = pl.pallas_call(
        functools.partial(exchange_kernel, sizes),
        in_specs=[vmem] * 4,
        out_specs=vmem,
        out_shape=jax.ShapeDtypeStruct(partial_value.shape, bf16),
        scratch_shapes=[
            pltpu.VMEM((chips, block, cdev, LANES), bf16),
            pltpu.VMEM((chips, block, cdev, LANES), bf16),
            pltpu.VMEM((chips - 1, block, cdev, LANES), bf16),
            pltpu.VMEM((block, cdev, LANES), bf16),
            pltpu.VMEM((nvar, part, cdev, LANES), bf16),
            pltpu.VMEM((nvar, part, cdev, LANES), bf16),
            dma((chips,)), dma((chips,)),
            dma((chips - 1,)), dma((chips - 1,)),
            dma((nvar - 1,)), dma((nvar - 1,)),
            dma((nvar - 1,)), dma((nvar - 1,)),
            dma((chips - 1,)), dma((chips - 1,)),
            dma((chips,)), dma((chips,)),
        ],
        compiler_params=pltpu.CompilerParams(
            collective_id=0, has_side_effects=True, vmem_limit_bytes=40 * 2**20
        ),
        name="exchange",
    )(partial_value, win, bias_in.reshape(2 * hid, 1), wout)

    rtab = lat_inverse(lat_first, latdev)
    rtab = rtab.transpose(0, 2, 3, 1).reshape(2 * latdev, 2 * MLAT)
    htab = lon_inverse(lon_first, londev)
    htab = jnp.pad(htab, ((0, 0), (0, LANES - MLON), (0, 0))).reshape(2 * LANES, londev)
    field, summed, squared = pl.pallas_call(
        inverse_kernel,
        grid=(cdev // step,),
        in_specs=[
            pl.BlockSpec((2 * MLAT, step, LANES), lambda i: (0, i, 0)),
            pl.BlockSpec(rtab.shape, lambda i: (0, 0)),
            pl.BlockSpec(htab.shape, lambda i: (0, 0)),
        ],
        out_specs=[
            pl.BlockSpec((step, latdev, londev), lambda i: (i, 0, 0)),
            pl.BlockSpec((step, latdev), lambda i: (i, 0)),
            pl.BlockSpec((step, latdev), lambda i: (i, 0)),
        ],
        out_shape=[
            jax.ShapeDtypeStruct((cdev, latdev, londev), bf16),
            jax.ShapeDtypeStruct((cdev, latdev), jnp.float32),
            jax.ShapeDtypeStruct((cdev, latdev), jnp.float32),
        ],
        compiler_params=pltpu.CompilerParams(vmem_limit_bytes=40 * 2**20),
        name="inverse",
    )(whole, rtab, htab)

    local = jnp.sum(squared * area_weights(lat_first, latdev)[None, :], axis=1)
    packed = jnp.concatenate(
        [summed, jnp.broadcast_to(local[:, None], (cdev, LANES - latdev))], axis=1
    )
    zonal, energy = pl.pallas_call(
        functools.partial(statistics_kernel, sizes),
        in_specs=[vmem],
        out_specs=[vmem, vmem],
        out_shape=[jax.ShapeDtypeStruct((cdev, LANES), jnp.float32)] * 2,
        scratch_shapes=[
            pltpu.VMEM((nlat * nlon - 1, cdev, LANES), jnp.float32),
            dma((nlat * nlon - 1,)), dma((nlat * nlon - 1,)),
        ],
        compiler_params=pltpu.CompilerParams(collective_id=1, has_side_effects=True),
        name="statistics",
    )(packed)
    denominator = batch * LON * jnp.sum(area_weights(0, LAT))
    return (field[None], zonal[None, :, :latdev] / LON, energy[:, latdev] / denominator)


def solution(mesh):
    sizes = tuple(mesh.shape[name] for name in ("var", "lat", "lon"))
    nvar, nlat, nlon = sizes

    def body(state, weights_in, bias_in, weights_out):
        batch, cdev, latdev, _ = state.shape
        fits = (
            batch == 1
            and nlat % 2 == 0
            and MLAT % (nlat * nlon * nvar) == 0
            and cdev % 16 == 0
            and latdev < LANES
            and MLON <= LANES
        )
        if fits:
            return kernel_body(sizes, state, weights_in, bias_in, weights_out)
        return plain_body(state, weights_in, bias_in, weights_out)

    return jax.shard_map(
        body,
        mesh=mesh,
        in_specs=(P(None, "var", "lat", "lon"), P(), P(), P()),
        out_specs=(P(None, "var", "lat", "lon"), P(None, "var", "lat"), P("var")),
        check_vma=False,
    )
```

```python
import functools
import math

import jax
import jax.numpy as jnp
from jax import lax
from jax.experimental import pallas as pl
from jax.experimental.pallas import tpu as pltpu
from jax.sharding import PartitionSpec as P

LAT = 384
LON = 1024
MLAT = 96
MLON = 96


def lon_forward(first, count):
    index = first + jnp.arange(count, dtype=jnp.int32)
    modes = jnp.arange(MLON, dtype=jnp.int32)
    phase = index[:, None] * modes[None, :] % LON
    angle = phase.astype(jnp.float32) * (2.0 * math.pi / LON)
    scale = 1.0 / math.sqrt(LAT * LON)
    return (jnp.stack([jnp.cos(angle), -jnp.sin(angle)], 1) * scale).astype(jnp.bfloat16)


def lat_forward(first, count):
    freqs = jnp.arange(MLAT, dtype=jnp.int32) - MLAT // 2
    index = first + jnp.arange(count, dtype=jnp.int32)
    phase = jnp.mod(freqs[:, None] * index[None, :], LAT)
    angle = phase.astype(jnp.float32) * (2.0 * math.pi / LAT)
    cosine, sine = (jnp.cos(angle), jnp.sin(angle))
    return jnp.stack([jnp.stack([cosine, sine]), jnp.stack([-sine, cosine])])


def lat_inverse(first, count):
    freqs = jnp.arange(MLAT, dtype=jnp.int32) - MLAT // 2
    index = first + jnp.arange(count, dtype=jnp.int32)
    phase = jnp.mod(index[:, None] * freqs[None, :], LAT)
    angle = phase.astype(jnp.float32) * (2.0 * math.pi / LAT)
    cosine, sine = (jnp.cos(angle), jnp.sin(angle))
    return jnp.stack([jnp.stack([cosine, -sine]), jnp.stack([sine, cosine])]).astype(jnp.bfloat16)


def lon_inverse(first, count):
    modes = jnp.arange(MLON, dtype=jnp.int32)
    index = first + jnp.arange(count, dtype=jnp.int32)
    phase = modes[:, None] * index[None, :] % LON
    angle = phase.astype(jnp.float32) * (2.0 * math.pi / LON)
    factor = jnp.where(modes == 0, 1.0, 2.0).astype(jnp.float32)[:, None] / math.sqrt(LAT * LON)
    return jnp.stack([factor * jnp.cos(angle), -factor * jnp.sin(angle)]).astype(jnp.bfloat16)


def area_weights(first, count):
    index = first + jnp.arange(count, dtype=jnp.int32)
    return jnp.cos(math.pi * ((index.astype(jnp.float32) + 0.5) / LAT - 0.5))


def complex_block(pair):
    real_part, imag_part = (pair[0], pair[1])
    return jnp.stack(
        [jnp.stack([real_part, -imag_part], 1), jnp.stack([imag_part, real_part], 1)], 0
    )


def plain_body(state, weights_in, bias_in, weights_out):
    batch, cdev, latdev, londev = state.shape
    nlat = lax.axis_size("lat")
    nlon = lax.axis_size("lon")
    lat_first = lax.axis_index("lat") * latdev
    lon_first = lax.axis_index("lon") * londev
    modes_lat = MLAT // nlat
    modes_lon = MLON // nlon
    qtab = lat_forward(lat_first, latdev)
    qsplit = qtab.reshape(2, 2, nlat, modes_lat, latdev)
    lonpart = jnp.einsum(
        "bcnl,lpk->pbcnk", state, lon_forward(lon_first, londev), preferred_element_type=jnp.float32
    )
    lonsplit = lonpart.reshape(2, batch, cdev, latdev, nlon, modes_lon)
    partial_value = jnp.einsum(
        "qpIJn,pbcnKk->qbcIKJk", qsplit, lonsplit, precision=lax.Precision.HIGHEST
    )
    spectrum = lax.psum_scatter(
        partial_value.reshape(2, batch, cdev, -1), ("lat", "lon"), scatter_dimension=3, tiled=True
    )
    spectrum = spectrum.astype(jnp.bfloat16)
    block_in = complex_block(weights_in)
    block_out = complex_block(weights_out)
    whole = lax.all_gather(spectrum, "var", axis=2, tiled=True)
    owned = lax.dynamic_slice_in_dim(block_out, lax.axis_index("var") * cdev, cdev, 1)
    hidden = jnp.einsum("qhpc,pbcj->qbhj", block_in, whole, preferred_element_type=jnp.float32)
    hidden = jnp.maximum(hidden + bias_in[:, None, :, None], 0.0).astype(jnp.bfloat16)
    mixed = jnp.einsum("qoph,pbhj->qboj", owned, hidden, preferred_element_type=jnp.float32).astype(
        jnp.bfloat16
    )
    mixed = mixed.reshape(2, batch, cdev, modes_lat, modes_lon)
    rtab = lat_inverse(lat_first, latdev)
    table = rtab
    latback = jnp.einsum(
        "qpnj,pbcjk->qbcnk",
        table,
        lax.all_gather(mixed, "lat", axis=3, tiled=True),
        preferred_element_type=jnp.float32,
    ).astype(jnp.bfloat16)
    htab = lon_inverse(lon_first, londev)
    table = htab
    result = jnp.einsum(
        "pbcnk,pkl->bcnl",
        lax.all_gather(latback, "lon", axis=4, tiled=True),
        table,
        preferred_element_type=jnp.float32,
    )
    active = jax.nn.gelu(result, approximate=False)
    field = active.astype(jnp.bfloat16)
    weights = area_weights(lat_first, latdev)
    denominator = batch * LON * jnp.sum(area_weights(0, LAT))
    row_total = jnp.sum(active, -1)
    row_square = jnp.sum(active * active, -1)
    summed, squared = lax.psum((row_total, row_square), "lon")
    zonal = summed / LON
    local = jnp.sum(squared * weights[None, None, :], axis=(0, 2))
    energy = lax.psum(local, "lat") / denominator
    return (field, zonal, energy)

LANES = 128
MESH = pl.DeviceIdType.MESH


def pad_lanes(table):
    return jnp.pad(table, [(0, 0)] * (table.ndim - 1) + [(0, LANES - table.shape[-1])])


def forward_kernel(x_ref, e_ref, q_ref, out_ref):
    channels, rows, count = x_ref.shape
    lon = jnp.dot(
        x_ref[...].reshape(channels * rows, count), e_ref[...], preferred_element_type=jnp.float32
    ).astype(jnp.bfloat16)
    lon = lon.reshape(channels, rows, 2 * LANES)
    parts = []
    for c in range(channels):
        both = jnp.concatenate([lon[c, :, :LANES], lon[c, :, LANES:]], 0)
        parts.append(jnp.dot(q_ref[...], both, preferred_element_type=jnp.float32))
    out_ref[...] = jnp.swapaxes(jnp.stack(parts), 0, 1).astype(jnp.bfloat16)


def inverse_kernel(g_ref, r_ref, h_ref, field_ref, zonal_ref, square_ref):
    channels = g_ref.shape[1]
    rows = field_ref.shape[1]
    modes = jnp.swapaxes(g_ref[...].astype(jnp.float32), 0, 1).astype(jnp.bfloat16)
    for c in range(channels):
        lat = jnp.dot(r_ref[...], modes[c], preferred_element_type=jnp.float32).astype(jnp.bfloat16)
        both = jnp.concatenate([lat[:rows], lat[rows:]], 1)
        result = jnp.dot(both, h_ref[...], preferred_element_type=jnp.float32)
        active = (0.5 * result) * (1.0 + lax.erf(result * math.sqrt(0.5)))
        field_ref[c] = active.astype(jnp.bfloat16)
        zonal_ref[c, :] = jnp.sum(active, -1)
        square_ref[c, :] = jnp.sum(active * active, -1)


def exchange_kernel(
    sizes, p_ref, win_ref, bias_ref, wout_ref, out_ref,
    pair, sums, slots, spec, gathered, back,
    s_pair, r_pair, s_red, r_red, s_z, r_z, s_b, r_b, s_all, r_all, s_fwd, r_fwd,
):
    nvar, nlat, nlon = sizes
    v, lat, lon = lax.axis_index("var"), lax.axis_index("lat"), lax.axis_index("lon")
    upper, core = lat // 2, lax.rem(lat, 2)
    nupper = nlat // 2
    block = p_ref.shape[0] // (nlat * nlon)
    part = block // nvar
    offsets = [(a, b) for a in range(nupper) for b in range(nlon)]
    count = len(offsets)

    def chip(t, sign=1):
        a, b = offsets[t]
        return (
            lax.rem(upper + sign * a + nupper, nupper),
            lax.rem(lon + sign * b + nlon, nlon),
        )

    def rows(where, parity):
        a, b = where
        return pl.ds(((a * 2 + parity) * nlon + b) * block, block)

    def send(src, dst, ssem, rsem, target):
        return pltpu.make_async_remote_copy(
            src_ref=src, dst_ref=dst, send_sem=ssem, recv_sem=rsem,
            device_id=target, device_id_type=MESH,
        )

    sibling = {"lat": upper * 2 + 1 - core}

    def peer(t):
        a, b = chip(t)
        return {"lat": a * 2 + core, "lon": b}

    def other(d):
        return {"var": lax.rem(v + d, nvar)}

    barrier = pltpu.get_barrier_semaphore()
    targets = [sibling] + [peer(t) for t in range(1, count)] + [other(d) for d in range(1, nvar)]
    for target in targets:
        pl.semaphore_signal(barrier, inc=1, device_id=target, device_id_type=MESH)
    pl.semaphore_wait(barrier, len(targets))

    order = list(range(1, count))[::-1] + [0]
    pairs = {}
    for t in order:
        pairs[t] = send(
            p_ref.at[rows(chip(t), 1 - core)], pair.at[t], s_pair.at[t], r_pair.at[t], sibling
        )
        pairs[t].start()
    reds = {}
    for t in order:
        pairs[t].wait_recv()
        mine = p_ref[rows(chip(t), core)].astype(jnp.float32) + pair[t].astype(jnp.float32)
        sums[t] = mine.astype(jnp.bfloat16)
        if t:
            reds[t] = send(sums.at[t], slots.at[t - 1], s_red.at[t - 1], r_red.at[t - 1], peer(t))
            reds[t].start()
    for t in order[:-1]:
        reds[t].wait_recv()
    total = sums[0].astype(jnp.float32)
    for t in range(1, count):
        total = total + slots[t - 1].astype(jnp.float32)
    spec[...] = total.astype(jnp.bfloat16)
    zs = []
    for d in range(1, nvar):
        copy = send(
            spec.at[pl.ds(lax.rem(v + d, nvar) * part, part)], gathered.at[v],
            s_z.at[d - 1], r_z.at[d - 1], other(d),
        )
        copy.start()
        zs.append(copy)
    gathered[v] = spec[pl.ds(v * part, part)]
    for d in range(1, nvar):
        src = gathered.at[lax.rem(v - d + nvar, nvar)]
        send(src, src, s_z.at[d - 1], r_z.at[d - 1], other(d)).wait_recv()
    held = gathered[...]
    cdev = held.shape[2]
    real, imag = [
        jnp.concatenate(
            [held[:, 2 * j + q].reshape(nvar * cdev, LANES) for j in range(part // 2)], 1
        )
        for q in range(2)
    ]

    def product(a, b):
        return jnp.dot(a, b, preferred_element_type=jnp.float32)

    def mix(w_ref, a, b):
        return (
            product(w_ref[0], a) - product(w_ref[1], b),
            product(w_ref[1], a) + product(w_ref[0], b),
        )

    pair_in = mix(win_ref, real, imag)
    hidden = [jnp.maximum(pair_in[q] + bias_ref[q], 0.0).astype(jnp.bfloat16) for q in range(2)]
    mixed = mix(wout_ref, *hidden)
    for q in range(2):
        for j in range(part // 2):
            piece = mixed[q][:, j * LANES : (j + 1) * LANES].astype(jnp.bfloat16)
            back[:, 2 * j + q] = piece.reshape(nvar, cdev, LANES)
    base = (lat * nlon + lon) * block
    bs = []
    for d in range(1, nvar):
        copy = send(
            back.at[lax.rem(v + d, nvar)], out_ref.at[pl.ds(base + v * part, part)],
            s_b.at[d - 1], r_b.at[d - 1], other(d),
        )
        copy.start()
        bs.append(copy)
    out_ref[pl.ds(base + v * part, part)] = back[v]
    for d in range(1, nvar):
        src = out_ref.at[pl.ds(base + lax.rem(v - d + nvar, nvar) * part, part)]
        send(src, src, s_b.at[d - 1], r_b.at[d - 1], other(d)).wait_recv()
    own = out_ref.at[pl.ds(base, block)]
    alls = []
    for t in order[:-1]:
        copy = send(own, own, s_all.at[t - 1], r_all.at[t - 1], peer(t))
        copy.start()
        alls.append(copy)
    fwd = [send(own, own, s_fwd.at[0], r_fwd.at[0], sibling)]
    fwd[0].start()
    for t in range(1, count):
        got = out_ref.at[rows(chip(t, -1), core)]
        send(got, got, s_all.at[t - 1], r_all.at[t - 1], peer(t)).wait_recv()
        copy = send(got, got, s_fwd.at[t], r_fwd.at[t], sibling)
        copy.start()
        fwd.append(copy)
    for t in range(count):
        got = out_ref.at[rows(chip(t, -1), 1 - core)]
        send(got, got, s_fwd.at[t], r_fwd.at[t], sibling).wait_recv()
    for copy in list(pairs.values()) + list(reds.values()) + zs + bs + alls + fwd:
        copy.wait_send()


def statistics_kernel(sizes, x_ref, zonal_ref, energy_ref, slots, s_sem, r_sem):
    nvar, nlat, nlon = sizes
    lat, lon = lax.axis_index("lat"), lax.axis_index("lon")
    offsets = [(a, b) for a in range(nlat) for b in range(nlon)][1:]

    def target(t):
        a, b = offsets[t]
        return {"lat": lax.rem(lat + a, nlat), "lon": lax.rem(lon + b, nlon)}

    barrier = pltpu.get_barrier_semaphore()
    for t in range(len(offsets)):
        pl.semaphore_signal(barrier, inc=1, device_id=target(t), device_id_type=MESH)
    pl.semaphore_wait(barrier, len(offsets))
    copies = []
    for t in range(len(offsets)):
        copy = pltpu.make_async_remote_copy(
            src_ref=x_ref, dst_ref=slots.at[t], send_sem=s_sem.at[t], recv_sem=r_sem.at[t],
            device_id=target(t), device_id_type=MESH,
        )
        copy.start()
        copies.append(copy)
    zonal = x_ref[...]
    energy = x_ref[...]
    for t, (a, _) in enumerate(offsets):
        copies[t].wait_recv()
        energy = energy + slots[t]
        if a == 0:
            zonal = zonal + slots[t]
    zonal_ref[...] = zonal
    energy_ref[...] = energy
    for copy in copies:
        copy.wait_send()


def kernel_body(sizes, state, weights_in, bias_in, weights_out):
    nvar, nlat, nlon = sizes
    batch, cdev, latdev, londev = state.shape
    lat_first = lax.axis_index("lat") * latdev
    lon_first = lax.axis_index("lon") * londev
    vmem = pl.BlockSpec(memory_space=pltpu.VMEM)
    step = 16
    bf16 = jnp.bfloat16
    etab = pad_lanes(lon_forward(lon_first, londev)).reshape(londev, 2 * LANES)
    qtab = lat_forward(lat_first, latdev).astype(bf16)
    qtab = qtab.transpose(2, 0, 1, 3).reshape(2 * MLAT, 2 * latdev)
    partial_value = pl.pallas_call(
        forward_kernel,
        grid=(cdev // step,),
        in_specs=[
            pl.BlockSpec((step, latdev, londev), lambda i: (i, 0, 0)),
            pl.BlockSpec(etab.shape, lambda i: (0, 0)),
            pl.BlockSpec(qtab.shape, lambda i: (0, 0)),
        ],
        out_specs=pl.BlockSpec((2 * MLAT, step, LANES), lambda i: (0, i, 0)),
        out_shape=jax.ShapeDtypeStruct((2 * MLAT, cdev, LANES), bf16),
        compiler_params=pltpu.CompilerParams(vmem_limit_bytes=40 * 2**20),
        name="forward",
    )(state[0], etab, qtab)

    chips = nlat * nlon // 2
    block = 2 * MLAT // (nlat * nlon)
    part = block // nvar
    dma = pltpu.SemaphoreType.DMA
    whole = pl.pallas_call(
        functools.partial(exchange_kernel, sizes),
        in_specs=[vmem] * 4,
        out_specs=vmem,
        out_shape=jax.ShapeDtypeStruct(partial_value.shape, bf16),
        scratch_shapes=[
            pltpu.VMEM((chips, block, cdev, LANES), bf16),
            pltpu.VMEM((chips, block, cdev, LANES), bf16),
            pltpu.VMEM((chips - 1, block, cdev, LANES), bf16),
            pltpu.VMEM((block, cdev, LANES), bf16),
            pltpu.VMEM((nvar, part, cdev, LANES), bf16),
            pltpu.VMEM((nvar, part, cdev, LANES), bf16),
            dma((chips,)), dma((chips,)),
            dma((chips - 1,)), dma((chips - 1,)),
            dma((nvar - 1,)), dma((nvar - 1,)),
            dma((nvar - 1,)), dma((nvar - 1,)),
            dma((chips - 1,)), dma((chips - 1,)),
            dma((chips,)), dma((chips,)),
        ],
        compiler_params=pltpu.CompilerParams(
            collective_id=0, has_side_effects=True, vmem_limit_bytes=40 * 2**20
        ),
        name="exchange",
    )(partial_value, weights_in, bias_in[:, :, None], weights_out)

    rtab = lat_inverse(lat_first, latdev)
    rtab = rtab.transpose(0, 2, 3, 1).reshape(2 * latdev, 2 * MLAT)
    htab = lon_inverse(lon_first, londev)
    htab = jnp.pad(htab, ((0, 0), (0, LANES - MLON), (0, 0))).reshape(2 * LANES, londev)
    field, summed, squared = pl.pallas_call(
        inverse_kernel,
        grid=(cdev // step,),
        in_specs=[
            pl.BlockSpec((2 * MLAT, step, LANES), lambda i: (0, i, 0)),
            pl.BlockSpec(rtab.shape, lambda i: (0, 0)),
            pl.BlockSpec(htab.shape, lambda i: (0, 0)),
        ],
        out_specs=[
            pl.BlockSpec((step, latdev, londev), lambda i: (i, 0, 0)),
            pl.BlockSpec((step, latdev), lambda i: (i, 0)),
            pl.BlockSpec((step, latdev), lambda i: (i, 0)),
        ],
        out_shape=[
            jax.ShapeDtypeStruct((cdev, latdev, londev), bf16),
            jax.ShapeDtypeStruct((cdev, latdev), jnp.float32),
            jax.ShapeDtypeStruct((cdev, latdev), jnp.float32),
        ],
        compiler_params=pltpu.CompilerParams(vmem_limit_bytes=40 * 2**20),
        name="inverse",
    )(whole, rtab, htab)

    local = jnp.sum(squared * area_weights(lat_first, latdev)[None, :], axis=1)
    packed = jnp.concatenate(
        [summed, jnp.broadcast_to(local[:, None], (cdev, LANES - latdev))], axis=1
    )
    zonal, energy = pl.pallas_call(
        functools.partial(statistics_kernel, sizes),
        in_specs=[vmem],
        out_specs=[vmem, vmem],
        out_shape=[jax.ShapeDtypeStruct((cdev, LANES), jnp.float32)] * 2,
        scratch_shapes=[
            pltpu.VMEM((nlat * nlon - 1, cdev, LANES), jnp.float32),
            dma((nlat * nlon - 1,)), dma((nlat * nlon - 1,)),
        ],
        compiler_params=pltpu.CompilerParams(collective_id=1, has_side_effects=True),
        name="statistics",
    )(packed)
    denominator = batch * LON * jnp.sum(area_weights(0, LAT))
    return (field[None], zonal[None, :, :latdev] / LON, energy[:, latdev] / denominator)


def solution(mesh):
    sizes = tuple(mesh.shape[name] for name in ("var", "lat", "lon"))
    nvar, nlat, nlon = sizes

    def body(state, weights_in, bias_in, weights_out):
        batch, cdev, latdev, _ = state.shape
        fits = (
            batch == 1
            and nlat % 2 == 0
            and MLAT % (nlat * nlon * nvar) == 0
            and cdev % 16 == 0
            and latdev < LANES
            and MLON <= LANES
        )
        if fits:
            return kernel_body(sizes, state, weights_in, bias_in, weights_out)
        return plain_body(state, weights_in, bias_in, weights_out)

    return jax.shard_map(
        body,
        mesh=mesh,
        in_specs=(P(None, "var", "lat", "lon"), P(), P(), P()),
        out_specs=(P(None, "var", "lat", "lon"), P(None, "var", "lat"), P("var")),
        check_vma=False,
    )
```
